32 devices in a mesh: row: 8 (over y, x, core), shift: 4 (over z).
Axes of the slice: x: 2, y: 2, z: 4, core: 2. Of those that a mesh axis runs over, the one named last changes fastest.
Arguments:
- snapshots: bfloat16 [4096, 2, 128], P('row'), may hold values from -6 to 6
- tail_sensors: bfloat16 [128, 2, 128], replicated, may hold values from -6 to 6
- shift_offsets: int32 [12], P('shift'), may hold values from 0 to 128
- start_basis: float32 [64, 4096], P(None, 'row'), may hold values from -0.09375 to 0.09375
Outputs:
- covariance: float32 [4096, 4096], P('row', 'shift')
- signal_basis: float32 [64, 4096], P(None, 'row')
The draws below stay inside these ranges and needn't reach their ends.
Inputs may be any that keep to these rules, and one draw needn't show every extreme that they name: `shift_offsets`: each shift's first sensor.
All inputs are finite; a program needn't handle non-finite values.
Results may differ from the reference program's by a relative error of at most 0.0031.
Values may be sent and summed in bfloat16 or wider, within the bound.
A program may use at most 64 MiB of HBM per device.

```python
import jax
import jax.numpy as jnp
from jax import lax

M = 4096
K = 64
SNAPS = 128
TAIL = 128
ITERS = 2
SHIFTS = 12


def place_ends(drawn, stream_key, smallest, largest):
    longest = drawn.shape.index(max(drawn.shape))
    spots = []
    for shift in (0, 1):
        where = [jax.random.randint(jax.random.fold_in(stream_key, axis), (), 0, length) for axis, length in enumerate(drawn.shape)]
        where[longest] = (where[longest] + shift) % drawn.shape[longest]
        spots.append(tuple(where))
    return drawn.at[spots[0]].set(smallest).at[spots[1]].set(largest)


def level_of(rng, dims, split, low, high):
    factor_of, own = 1.0, jax.random.fold_in(rng, 6)
    for position, parts in split:
        draws = jnp.exp(jax.random.uniform(jax.random.fold_in(own, position), (parts,), jnp.float32, low / len(split), high / len(split)))
        factor_of = factor_of * jnp.repeat(draws, dims[position] // parts).reshape([-1 if axis == position else 1 for axis in range(len(dims))])
    return factor_of


def normal_values(stream_key, shape, scale, limit, split=(), held_as=jnp.bfloat16):
    factor_of = level_of(stream_key, shape, split, -0.22, 0.18) if split else 1.0
    entries = jax.random.normal(stream_key, shape, jnp.float32) * scale * factor_of
    return jnp.minimum(jnp.maximum(entries, -limit), limit).astype(held_as)


def setup_inputs(seed: int = 0) -> dict:
    splits = jax.random.split(jax.random.key(seed), 5)
    return {
        "snapshots": normal_values(splits[0], (M, 2, SNAPS), 0.7071, 6.0, ((0, 8),)),
        "tail_sensors": normal_values(splits[1], (TAIL, 2, SNAPS), 0.7071, 6.0),
        "shift_offsets": place_ends(jax.random.randint(splits[2], (SHIFTS,), 0, TAIL + 1), jax.random.fold_in(splits[2], 1), 0, TAIL).astype(jnp.int32),
        "start_basis": normal_values(splits[3], (K, M), M ** -0.5, 0.09375, ((1, 8),), jnp.float32),
    }


half_root = 0.7071067811865476

def make_rows(extended, offset):
    window = lax.dynamic_slice_in_dim(extended, offset, M, 0).astype(jnp.float32)
    mirror = window[::-1]
    summed_pair = window + mirror
    difference = window - mirror
    half_rows = M // 2
    upper_rows = jnp.concatenate([summed_pair[:half_rows, 0], summed_pair[:half_rows, 1]], axis=1)
    bottom = jnp.concatenate([difference[half_rows:, 1], -difference[half_rows:, 0]], axis=1)
    return (jnp.concatenate([upper_rows, bottom], 0) * half_root).astype(jnp.bfloat16)

def factor(gram_matrix):
    lower_factor = jnp.linalg.cholesky(gram_matrix)
    identity = jnp.eye(gram_matrix.shape[0], dtype=jnp.float32)
    return jax.scipy.linalg.solve_triangular(lower_factor, identity, lower=True)

def reference(snapshots, tail_sensors, shift_offsets, start_basis):
    extended = jnp.concatenate([snapshots, tail_sensors], 0)

    def add_shift(running, offset):
        pair_rows = make_rows(extended, offset)
        return (running + jnp.dot(pair_rows.astype(jnp.float32), pair_rows.T.astype(jnp.float32), preferred_element_type=jnp.float32), None)
    covariance_sum, unused = lax.scan(add_shift, jnp.zeros((M, M), jnp.float32), shift_offsets)
    covariance = covariance_sum * (1.0 / (SNAPS * SHIFTS))
    basis_rows = start_basis
    for sweep in range(ITERS):
        mapped = lax.dot_general(basis_rows, covariance, (((1,), (1,)), ((), ())), precision=lax.Precision.HIGHEST)
        gram_matrix = jnp.dot(mapped, mapped.T, precision=lax.Precision.HIGHEST)
        basis_rows = jnp.dot(factor(gram_matrix), mapped, precision=lax.Precision.HIGHEST)
    return (covariance, basis_rows)
```

```python
import functools

import jax
import jax.numpy as jnp
from jax import lax
from jax.experimental import pallas as pl
from jax.experimental.pallas import tpu as pltpu
from jax.sharding import PartitionSpec as P

MESH = pl.DeviceIdType.MESH
HALF_ROOT = 0.7071067811865476
NT = (((1,), (1,)), ((), ()))
NN = (((1,), (0,)), ((), ()))
CHUNK = 128


def split(value):
    high = value.astype(jnp.bfloat16)
    return high, (value - high.astype(jnp.float32)).astype(jnp.bfloat16)


def dot(left, right, dims):
    return lax.dot_general(left, right, dims, preferred_element_type=jnp.float32)


def dot3(left, right, dims):
    left_high, left_low = split(left)
    right_high, right_low = split(right)
    return dot(left_high, right_high, dims) + (
        dot(left_low, right_high, dims) + dot(left_high, right_low, dims)
    )


def dot_full(left, right, dims):
    return lax.dot_general(
        left,
        right,
        dims,
        precision=lax.Precision.HIGHEST,
        preferred_element_type=jnp.float32,
    )


def inverse_factor(gram):
    k = gram.shape[0]
    row_ids = lax.broadcasted_iota(jnp.int32, (k, k), 0)
    col_ids = lax.broadcasted_iota(jnp.int32, (k, k), 1)
    eye = jnp.where(row_ids == col_ids, 1.0, 0.0).astype(jnp.float32)
    table = jnp.concatenate([gram, eye], axis=1)
    tall = lax.broadcasted_iota(jnp.int32, (k, 2 * k), 0)
    for j in range(k - 1):
        pivot_row = table[j : j + 1, :]
        scaled = pivot_row * (1.0 / table[j : j + 1, j : j + 1])
        column = jnp.broadcast_to(table[:, j : j + 1], (k, 2 * k))
        table = table - jnp.where(tall > j, column * scaled, 0.0)
    pivots = jnp.sum(jnp.where(row_ids == col_ids, table[:, :k], 0.0), axis=1, keepdims=True)
    return table[:, k:] * lax.rsqrt(pivots)


def kernel(
    n_row, n_shift, m,
    snap_ref, tail_ref, offs_ref, start_ref,
    cov_ref, basis_ref,
    xb, xf, rf, prow, pcol, cov, offs_v, offs_s,
    t1, rs1, ag1, t2, rs2, ag2, g1, g2,
    x_send, x_fwd, x_recv, o_send, o_recv,
    rs1_send, rs1_recv, ag1_send, ag1_recv,
    rs2_send, rs2_recv, ag2_send, ag2_recv,
    g1_send, g1_recv, g2_send, g2_recv, local_sem, cov_sem,
):
    me = lax.axis_index("row")
    col = lax.axis_index("shift")
    rows = snap_ref.shape[0]
    tail = tail_ref.shape[0]
    k = start_ref.shape[0]
    cols = m // n_shift
    pair = me % 2
    mate = me + 1 - 2 * pair

    barrier = pltpu.get_barrier_semaphore()
    for d in range(1, n_row):
        pl.semaphore_signal(barrier, inc=1, device_id={"row": (me + d) % n_row}, device_id_type=MESH)
    for d in range(1, n_shift):
        pl.semaphore_signal(barrier, inc=1, device_id={"shift": (col + d) % n_shift}, device_id_type=MESH)
    pl.semaphore_wait(barrier, n_row + n_shift - 2)

    sends = []

    def remote(src, dst, send, recv, axis, index):
        return pltpu.make_async_remote_copy(
            src_ref=src, dst_ref=dst, send_sem=send, recv_sem=recv,
            device_id={axis: index}, device_id_type=MESH,
        )

    def push(*args):
        copy = remote(*args)
        copy.start()
        sends.append(copy)

    def block(index):
        return xb.at[pl.ds(pl.multiple_of(index * rows, rows), rows)]

    for d in range(1, n_shift):
        push(offs_ref, offs_v.at[col], o_send.at[d], o_recv.at[col], "shift", (col + d) % n_shift)
    for d in range(1, n_row // 2):
        push(snap_ref, block(me), x_send.at[d], x_recv.at[me], "row", (me + 2 * d) % n_row)
    push(snap_ref, block(me), x_send.at[0], x_recv.at[me], "row", mate)
    own_copy = pltpu.make_async_copy(snap_ref, block(me), local_sem.at[0])
    own_copy.start()
    tail_copy = pltpu.make_async_copy(tail_ref, xb.at[pl.ds(m, tail)], local_sem.at[1])
    tail_copy.start()

    flip_rows = lax.broadcasted_iota(jnp.int32, (CHUNK, CHUNK), 0)
    flip_cols = lax.broadcasted_iota(jnp.int32, (CHUNK, CHUNK), 1)
    flip = jnp.where(flip_rows + flip_cols == CHUNK - 1, 1.0, 0.0).astype(jnp.bfloat16)

    def spread(first, count):
        def one(c, carry):
            at = pl.multiple_of(first + c * CHUNK, CHUNK)
            value = xb[pl.ds(at, CHUNK), :]
            plain = value.astype(jnp.float32)
            back = dot(flip, value, NN)
            other = pl.multiple_of(m + tail - CHUNK - at, CHUNK)
            half = plain.shape[1] // 2
            xf[0, pl.ds(at, CHUNK), :] = plain[:, :half]
            xf[1, pl.ds(at, CHUNK), :] = plain[:, half:]
            rf[0, pl.ds(other, CHUNK), :] = back[:, :half]
            rf[1, pl.ds(other, CHUNK), :] = back[:, half:]
            return carry

        lax.fori_loop(0, count // CHUNK, one, 0)

    tail_copy.wait()
    spread(m, tail)
    own_copy.wait()
    for d in range(n_row // 2):
        src = (me + n_row - 2 * d) % n_row
        if d:
            remote(snap_ref, block(src), x_send.at[d], x_recv.at[src], "row", src).wait_recv()
            push(block(src), block(src), x_fwd.at[d], x_recv.at[src], "row", mate)
        spread(src * rows, rows)
    for d in range(n_row // 2):
        src = (mate + n_row - 2 * d) % n_row
        remote(snap_ref, block(src), x_send.at[d], x_recv.at[src], "row", mate).wait_recv()
        spread(src * rows, rows)

    offs_v[col] = offs_ref[...]
    for d in range(1, n_shift):
        src = (col + n_shift - d) % n_shift
        remote(offs_ref, offs_v.at[src], o_send.at[d], o_recv.at[src], "shift", src).wait_recv()
    to_scalar = pltpu.make_async_copy(offs_v, offs_s, local_sem.at[2])
    to_scalar.start()
    to_scalar.wait()

    snaps = xf.shape[2]
    width = 2 * snaps
    per = prow.shape[1] // (width * n_shift)

    def fill(target, start, count):
        lower = start >= m // 2
        first = jnp.where(lower, 1, 0)
        second = 1 - first
        sign = jnp.where(lower, -1.0, 1.0).astype(jnp.float32)

        def one_shift(s, carry):
            offset = offs_s[s // per, 0, s % per]
            lanes = pl.multiple_of(s * width, width)
            for c in range(count // CHUNK):
                near = pl.ds(offset + start + c * CHUNK, CHUNK)
                far = pl.ds(tail - offset + start + c * CHUNK, CHUNK)
                left = (xf[first, near, :] + sign * rf[first, far, :]) * HALF_ROOT
                right = (xf[second, near, :] + sign * rf[second, far, :]) * (sign * HALF_ROOT)
                target[pl.ds(c * CHUNK, CHUNK), pl.ds(lanes, snaps)] = left.astype(jnp.bfloat16)
                target[pl.ds(c * CHUNK, CHUNK), pl.ds(pl.multiple_of(lanes + snaps, snaps), snaps)] = right.astype(jnp.bfloat16)
            return carry

        lax.fori_loop(0, per * n_shift, one_shift, 0)

    fill(prow, me * rows, rows)
    fill(pcol, col * cols, cols)

    normalizer = 1.0 / (snaps * per * n_shift)
    tile = 256

    def one_tile(c, carry):
        at = pl.multiple_of(c * tile, tile)
        cov[:, pl.ds(at, tile)] = dot(prow[...], pcol[pl.ds(at, tile), :], NT) * normalizer
        return carry

    lax.fori_loop(0, cols // tile, one_tile, 0)
    cov_copy = pltpu.make_async_copy(cov, cov_ref, cov_sem)
    cov_copy.start()

    def scatter(value, out, landing, send, recv, axis, index, n):
        piece = k // n
        for p in range(n):
            out[p] = value[p * piece : (p + 1) * piece, :]
        for d in range(1, n):
            p = (index + d) % n
            push(out.at[p], landing.at[index], send.at[d], recv.at[index], axis, p)

    def collect(out, landing, held, send, recv, send2, recv2, axis, index, n):
        for d in range(1, n):
            p = (index + n - d) % n
            remote(out.at[p], landing.at[p], send.at[d], recv.at[p], axis, p).wait_recv()
        landing[index] = out[index]
        total = landing[0]
        for p in range(1, n):
            total = total + landing[p]
        held[index] = total
        for d in range(1, n):
            p = (index + d) % n
            push(held.at[index], held.at[index], send2.at[d], recv2.at[index], axis, p)

    def arrive(held, send, recv, axis, index, n):
        for d in range(1, n):
            p = (index + n - d) % n
            remote(held.at[p], held.at[p], send.at[d], recv.at[p], axis, p).wait_recv()

    def whole(held, n):
        return jnp.concatenate([held[p] for p in range(n)], axis=0)

    scatter(dot3(start_ref[...], cov[...], NN), t1, rs1, rs1_send, rs1_recv, "row", me, n_row)
    collect(t1, rs1, ag1, rs1_send, rs1_recv, ag1_send, ag1_recv, "row", me, n_row)
    arrive(ag1, ag1_send, ag1_recv, "row", me, n_row)
    mapped = whole(ag1, n_row)

    g1[col] = dot_full(mapped, mapped, NT)
    for d in range(1, n_shift):
        push(g1.at[col], g1.at[col], g1_send.at[d], g1_recv.at[col], "shift", (col + d) % n_shift)
    scatter(dot3(mapped, cov[...], NT), t2, rs2, rs2_send, rs2_recv, "shift", col, n_shift)
    arrive(g1, g1_send, g1_recv, "shift", col, n_shift)
    collect(t2, rs2, ag2, rs2_send, rs2_recv, ag2_send, ag2_recv, "shift", col, n_shift)
    gram = g1[0]
    for p in range(1, n_shift):
        gram = gram + g1[p]
    first_inverse = inverse_factor(gram)
    arrive(ag2, ag2_send, ag2_recv, "shift", col, n_shift)
    mapped = dot_full(first_inverse, whole(ag2, n_shift), NN)

    g2[me] = dot_full(mapped, mapped, NT)
    for d in range(1, n_row):
        push(g2.at[me], g2.at[me], g2_send.at[d], g2_recv.at[me], "row", (me + d) % n_row)
    arrive(g2, g2_send, g2_recv, "row", me, n_row)
    gram = g2[0]
    for p in range(1, n_row):
        gram = gram + g2[p]
    basis_ref[...] = dot_full(inverse_factor(gram), mapped, NN)

    for copy in sends:
        copy.wait_send()
    cov_copy.wait()


def per_device(n_row, n_shift, m, snapshots, tail_sensors, shift_offsets, start_basis):
    rows = snapshots.shape[0]
    tail = tail_sensors.shape[0]
    k = start_basis.shape[0]
    cols = m // n_shift
    per = shift_offsets.shape[0]
    width = snapshots.shape[1] * snapshots.shape[2]
    offsets = jnp.pad(shift_offsets[None], ((0, 0), (0, 128 - per)))
    vmem = pl.BlockSpec(memory_space=pltpu.VMEM)
    f32, bf16 = jnp.float32, jnp.bfloat16
    dma = pltpu.SemaphoreType.DMA
    return pl.pallas_call(
        functools.partial(kernel, n_row, n_shift, m),
        out_shape=(
            jax.ShapeDtypeStruct((rows, cols), f32),
            jax.ShapeDtypeStruct((k, rows), f32),
        ),
        in_specs=[vmem] * 4,
        out_specs=(pl.BlockSpec(memory_space=pl.ANY), vmem),
        scratch_shapes=[
            pltpu.VMEM((m + tail, width), bf16),
            pltpu.VMEM((2, m + tail, width // 2), f32),
            pltpu.VMEM((2, m + tail, width // 2), f32),
            pltpu.VMEM((rows, width * per * n_shift), bf16),
            pltpu.VMEM((cols, width * per * n_shift), bf16),
            pltpu.VMEM((rows, cols), f32),
            pltpu.VMEM((n_shift, 1, 128), jnp.int32),
            pltpu.SMEM((n_shift, 1, 128), jnp.int32),
            pltpu.VMEM((n_row, k // n_row, cols), f32),
            pltpu.VMEM((n_row, k // n_row, cols), f32),
            pltpu.VMEM((n_row, k // n_row, cols), f32),
            pltpu.VMEM((n_shift, k // n_shift, rows), f32),
            pltpu.VMEM((n_shift, k // n_shift, rows), f32),
            pltpu.VMEM((n_shift, k // n_shift, rows), f32),
            pltpu.VMEM((n_shift, k, k), f32),
            pltpu.VMEM((n_row, k, k), f32),
            dma((n_row,)), dma((n_row,)), dma((n_row,)),
            dma((n_shift,)), dma((n_shift,)),
            dma((n_row,)), dma((n_row,)), dma((n_row,)), dma((n_row,)),
            dma((n_shift,)), dma((n_shift,)), dma((n_shift,)), dma((n_shift,)),
            dma((n_shift,)), dma((n_shift,)), dma((n_row,)), dma((n_row,)),
            dma((3,)), dma,
        ],
        compiler_params=pltpu.CompilerParams(
            collective_id=0, has_side_effects=True, vmem_limit_bytes=60000 * 1024
        ),
    )(snapshots.reshape(rows, width), tail_sensors.reshape(tail, width), offsets, start_basis)


def solution(mesh):
    n_row, n_shift = mesh.shape["row"], mesh.shape["shift"]

    def step(snapshots, tail_sensors, shift_offsets, start_basis):
        m = snapshots.shape[0]
        return jax.shard_map(
            functools.partial(per_device, n_row, n_shift, m),
            mesh=mesh,
            in_specs=(P("row", None, None), P(), P("shift"), P(None, "row")),
            out_specs=(P("row", "shift"), P(None, "row")),
            check_vma=False,
        )(snapshots, tail_sensors, shift_offsets, start_basis)

    return step
```

```python
import functools

import jax
import jax.numpy as jnp
from jax import lax
from jax.experimental import pallas as pl
from jax.experimental.pallas import tpu as pltpu
from jax.sharding import PartitionSpec as P

MESH = pl.DeviceIdType.MESH
HALF_ROOT = 0.7071067811865476
NT = (((1,), (1,)), ((), ()))
NN = (((1,), (0,)), ((), ()))
CHUNK = 128
GROUP = 8


def split(value):
    high = value.astype(jnp.bfloat16)
    return high, (value - high.astype(jnp.float32)).astype(jnp.bfloat16)


def dot(left, right, dims):
    return lax.dot_general(left, right, dims, preferred_element_type=jnp.float32)


def dot3(left, right, dims):
    left_high, left_low = split(left)
    right_high, right_low = split(right)
    return dot(left_high, right_high, dims) + (
        dot(left_low, right_high, dims) + dot(left_high, right_low, dims)
    )


def dot_full(left, right, dims):
    return lax.dot_general(
        left,
        right,
        dims,
        precision=lax.Precision.HIGHEST,
        preferred_element_type=jnp.float32,
    )


def inverse_factor(gram):
    k = gram.shape[0]
    row_ids = lax.broadcasted_iota(jnp.int32, (k, k), 0)
    col_ids = lax.broadcasted_iota(jnp.int32, (k, k), 1)
    eye = jnp.where(row_ids == col_ids, 1.0, 0.0).astype(jnp.float32)
    table = jnp.concatenate([gram, eye], axis=1)
    tall = lax.broadcasted_iota(jnp.int32, (k, 2 * k), 0)
    for j in range(0, k, GROUP):
        columns = [jnp.broadcast_to(table[:, j + a : j + a + 1], (k, 2 * k)) for a in range(GROUP)]
        rows = [table[j + a : j + a + 1, :] for a in range(GROUP)]
        for a in range(GROUP):
            inverse = 1.0 / columns[a][j + a : j + a + 1, :]
            scaled = rows[a] * inverse
            for c in range(a + 1, GROUP):
                shared = columns[a][j + c : j + c + 1, :]
                factor = columns[c][j + a : j + a + 1, :] * inverse
                columns[c] = columns[c] - columns[a] * factor
                rows[c] = rows[c] - scaled * shared
            table = table - jnp.where(tall > j + a, columns[a] * scaled, 0.0)
    pivots = jnp.sum(jnp.where(row_ids == col_ids, table[:, :k], 0.0), axis=1, keepdims=True)
    return table[:, k:] * lax.rsqrt(pivots)


def kernel(
    n_row, n_shift, m,
    snap_ref, tail_ref, offs_ref, start_ref,
    cov_ref, basis_ref,
    xb, xf, rf, prow, pcol, cov, offs_v, offs_s,
    t1, rs1, ag1, t2, rs2, ag2, g1, g2,
    x_send, x_fwd, x_recv, o_send, o_recv,
    rs1_send, rs1_recv, ag1_send, ag1_recv,
    rs2_send, rs2_recv, ag2_send, ag2_recv,
    g1_send, g1_recv, g2_send, g2_recv, local_sem, cov_sem,
):
    me = lax.axis_index("row")
    col = lax.axis_index("shift")
    rows = snap_ref.shape[0]
    tail = tail_ref.shape[0]
    k = start_ref.shape[0]
    cols = m // n_shift
    pair = me % 2
    mate = me + 1 - 2 * pair

    barrier = pltpu.get_barrier_semaphore()
    for d in range(1, n_row):
        pl.semaphore_signal(barrier, inc=1, device_id={"row": (me + d) % n_row}, device_id_type=MESH)
    for d in range(1, n_shift):
        pl.semaphore_signal(barrier, inc=1, device_id={"shift": (col + d) % n_shift}, device_id_type=MESH)
    pl.semaphore_wait(barrier, n_row + n_shift - 2)

    sends = []

    def remote(src, dst, send, recv, axis, index):
        return pltpu.make_async_remote_copy(
            src_ref=src, dst_ref=dst, send_sem=send, recv_sem=recv,
            device_id={axis: index}, device_id_type=MESH,
        )

    def push(*args):
        copy = remote(*args)
        copy.start()
        sends.append(copy)

    def block(index):
        return xb.at[pl.ds(pl.multiple_of(index * rows, rows), rows)]

    lanes_of = lax.broadcasted_iota(jnp.int32, (1, 128), 1)
    listed = jnp.zeros((1, 128), jnp.int32)
    for j in range(offs_ref.shape[0]):
        listed = jnp.where(lanes_of == j, offs_ref[j], listed)
    offs_v[col] = listed

    for d in range(1, n_shift):
        push(offs_v.at[col], offs_v.at[col], o_send.at[d], o_recv.at[col], "shift", (col + d) % n_shift)
    for d in range(1, n_row // 2):
        push(snap_ref, block(me), x_send.at[d], x_recv.at[me], "row", (me + 2 * d) % n_row)
    push(snap_ref, block(me), x_send.at[0], x_recv.at[me], "row", mate)
    own_copy = pltpu.make_async_copy(snap_ref, block(me), local_sem.at[0])
    own_copy.start()
    tail_copy = pltpu.make_async_copy(tail_ref, xb.at[pl.ds(m, tail)], local_sem.at[1])
    tail_copy.start()

    flip_rows = lax.broadcasted_iota(jnp.int32, (CHUNK, CHUNK), 0)
    flip_cols = lax.broadcasted_iota(jnp.int32, (CHUNK, CHUNK), 1)
    flip = jnp.where(flip_rows + flip_cols == CHUNK - 1, 1.0, 0.0).astype(jnp.bfloat16)

    def spread(first, count):
        def one(c, carry):
            at = pl.multiple_of(first + c * CHUNK, CHUNK)
            value = xb[pl.ds(at, CHUNK), :]
            plain = value.astype(jnp.float32)
            back = dot(flip, value, NN)
            other = pl.multiple_of(m + tail - CHUNK - at, CHUNK)
            half = plain.shape[1] // 2
            xf[0, pl.ds(at, CHUNK), :] = plain[:, :half]
            xf[1, pl.ds(at, CHUNK), :] = plain[:, half:]
            rf[0, pl.ds(other, CHUNK), :] = back[:, :half]
            rf[1, pl.ds(other, CHUNK), :] = back[:, half:]
            return carry

        lax.fori_loop(0, count // CHUNK, one, 0)

    tail_copy.wait()
    spread(m, tail)
    own_copy.wait()
    for d in range(n_row // 2):
        src = (me + n_row - 2 * d) % n_row
        if d:
            remote(snap_ref, block(src), x_send.at[d], x_recv.at[src], "row", src).wait_recv()
            push(block(src), block(src), x_fwd.at[d], x_recv.at[src], "row", mate)
        spread(src * rows, rows)
    for d in range(n_row // 2):
        src = (mate + n_row - 2 * d) % n_row
        remote(snap_ref, block(src), x_send.at[d], x_recv.at[src], "row", mate).wait_recv()
        spread(src * rows, rows)

    for d in range(1, n_shift):
        src = (col + n_shift - d) % n_shift
        remote(offs_v.at[src], offs_v.at[src], o_send.at[d], o_recv.at[src], "shift", src).wait_recv()
    to_scalar = pltpu.make_async_copy(offs_v, offs_s, local_sem.at[2])
    to_scalar.start()
    to_scalar.wait()

    snaps = xf.shape[2]
    width = 2 * snaps
    per = prow.shape[1] // (width * n_shift)

    def fill(target, start, count):
        lower = start >= m // 2
        first = jnp.where(lower, 1, 0)
        second = 1 - first
        sign = jnp.where(lower, -1.0, 1.0).astype(jnp.float32)

        def one_shift(s, carry):
            offset = offs_s[s // per, 0, s % per]
            lanes = pl.multiple_of(s * width, width)
            for c in range(count // CHUNK):
                near = pl.ds(offset + start + c * CHUNK, CHUNK)
                far = pl.ds(tail - offset + start + c * CHUNK, CHUNK)
                left = (xf[first, near, :] + sign * rf[first, far, :]) * HALF_ROOT
                right = (xf[second, near, :] + sign * rf[second, far, :]) * (sign * HALF_ROOT)
                target[pl.ds(c * CHUNK, CHUNK), pl.ds(lanes, snaps)] = left.astype(jnp.bfloat16)
                target[pl.ds(c * CHUNK, CHUNK), pl.ds(pl.multiple_of(lanes + snaps, snaps), snaps)] = right.astype(jnp.bfloat16)
            return carry

        lax.fori_loop(0, per * n_shift, one_shift, 0)

    fill(prow, me * rows, rows)
    fill(pcol, col * cols, cols)

    normalizer = 1.0 / (snaps * per * n_shift)
    tile = 256

    def one_tile(c, carry):
        at = pl.multiple_of(c * tile, tile)
        cov[:, pl.ds(at, tile)] = dot(prow[...], pcol[pl.ds(at, tile), :], NT) * normalizer
        return carry

    lax.fori_loop(0, cols // tile, one_tile, 0)
    cov_copy = pltpu.make_async_copy(cov, cov_ref, cov_sem)
    cov_copy.start()

    def scatter(value, out, landing, send, recv, axis, index, n):
        piece = k // n
        for p in range(n):
            out[p] = value[p * piece : (p + 1) * piece, :]
        for d in range(1, n):
            p = (index + d) % n
            push(out.at[p], landing.at[index], send.at[d], recv.at[index], axis, p)

    def collect(out, landing, held, send, recv, send2, recv2, axis, index, n):
        for d in range(1, n):
            p = (index + n - d) % n
            remote(out.at[p], landing.at[p], send.at[d], recv.at[p], axis, p).wait_recv()
        landing[index] = out[index]
        total = landing[0]
        for p in range(1, n):
            total = total + landing[p]
        held[index] = total
        for d in range(1, n):
            p = (index + d) % n
            push(held.at[index], held.at[index], send2.at[d], recv2.at[index], axis, p)

    def arrive(held, send, recv, axis, index, n):
        for d in range(1, n):
            p = (index + n - d) % n
            remote(held.at[p], held.at[p], send.at[d], recv.at[p], axis, p).wait_recv()

    def whole(held, n):
        return jnp.concatenate([held[p] for p in range(n)], axis=0)

    scatter(dot3(start_ref[...], cov[...], NN), t1, rs1, rs1_send, rs1_recv, "row", me, n_row)
    collect(t1, rs1, ag1, rs1_send, rs1_recv, ag1_send, ag1_recv, "row", me, n_row)
    arrive(ag1, ag1_send, ag1_recv, "row", me, n_row)
    mapped = whole(ag1, n_row)

    g1[col] = dot_full(mapped, mapped, NT)
    for d in range(1, n_shift):
        push(g1.at[col], g1.at[col], g1_send.at[d], g1_recv.at[col], "shift", (col + d) % n_shift)
    scatter(dot3(mapped, cov[...], NT), t2, rs2, rs2_send, rs2_recv, "shift", col, n_shift)
    arrive(g1, g1_send, g1_recv, "shift", col, n_shift)
    collect(t2, rs2, ag2, rs2_send, rs2_recv, ag2_send, ag2_recv, "shift", col, n_shift)
    gram = g1[0]
    for p in range(1, n_shift):
        gram = gram + g1[p]
    first_inverse = inverse_factor(gram)
    arrive(ag2, ag2_send, ag2_recv, "shift", col, n_shift)
    mapped = dot_full(first_inverse, whole(ag2, n_shift), NN)

    g2[me] = dot_full(mapped, mapped, NT)
    for d in range(1, n_row):
        push(g2.at[me], g2.at[me], g2_send.at[d], g2_recv.at[me], "row", (me + d) % n_row)
    arrive(g2, g2_send, g2_recv, "row", me, n_row)
    gram = g2[0]
    for p in range(1, n_row):
        gram = gram + g2[p]
    basis_ref[...] = dot_full(inverse_factor(gram), mapped, NN)

    for copy in sends:
        copy.wait_send()
    cov_copy.wait()


def per_device(n_row, n_shift, m, snapshots, tail_sensors, shift_offsets, start_basis):
    rows = snapshots.shape[0]
    tail = tail_sensors.shape[0]
    k = start_basis.shape[0]
    cols = m // n_shift
    per = shift_offsets.shape[0]
    width = snapshots.shape[1] * snapshots.shape[2]
    vmem = pl.BlockSpec(memory_space=pltpu.VMEM)
    f32, bf16 = jnp.float32, jnp.bfloat16
    dma = pltpu.SemaphoreType.DMA
    return pl.pallas_call(
        functools.partial(kernel, n_row, n_shift, m),
        out_shape=(
            jax.ShapeDtypeStruct((rows, cols), f32),
            jax.ShapeDtypeStruct((k, rows), f32),
        ),
        in_specs=[vmem, vmem, pl.BlockSpec(memory_space=pltpu.SMEM), vmem],
        out_specs=(pl.BlockSpec(memory_space=pl.ANY), vmem),
        scratch_shapes=[
            pltpu.VMEM((m + tail, width), bf16),
            pltpu.VMEM((2, m + tail, width // 2), f32),
            pltpu.VMEM((2, m + tail, width // 2), f32),
            pltpu.VMEM((rows, width * per * n_shift), bf16),
            pltpu.VMEM((cols, width * per * n_shift), bf16),
            pltpu.VMEM((rows, cols), f32),
            pltpu.VMEM((n_shift, 1, 128), jnp.int32),
            pltpu.SMEM((n_shift, 1, 128), jnp.int32),
            pltpu.VMEM((n_row, k // n_row, cols), f32),
            pltpu.VMEM((n_row, k // n_row, cols), f32),
            pltpu.VMEM((n_row, k // n_row, cols), f32),
            pltpu.VMEM((n_shift, k // n_shift, rows), f32),
            pltpu.VMEM((n_shift, k // n_shift, rows), f32),
            pltpu.VMEM((n_shift, k // n_shift, rows), f32),
            pltpu.VMEM((n_shift, k, k), f32),
            pltpu.VMEM((n_row, k, k), f32),
            dma((n_row,)), dma((n_row,)), dma((n_row,)),
            dma((n_shift,)), dma((n_shift,)),
            dma((n_row,)), dma((n_row,)), dma((n_row,)), dma((n_row,)),
            dma((n_shift,)), dma((n_shift,)), dma((n_shift,)), dma((n_shift,)),
            dma((n_shift,)), dma((n_shift,)), dma((n_row,)), dma((n_row,)),
            dma((3,)), dma,
        ],
        compiler_params=pltpu.CompilerParams(
            collective_id=0, has_side_effects=True, vmem_limit_bytes=32 * 1024 * 1024
        ),
    )(snapshots.reshape(rows, width), tail_sensors.reshape(tail, width), shift_offsets, start_basis)


def solution(mesh):
    n_row, n_shift = mesh.shape["row"], mesh.shape["shift"]

    def step(snapshots, tail_sensors, shift_offsets, start_basis):
        m = snapshots.shape[0]
        return jax.shard_map(
            functools.partial(per_device, n_row, n_shift, m),
            mesh=mesh,
            in_specs=(P("row", None, None), P(), P("shift"), P(None, "row")),
            out_specs=(P("row", "shift"), P(None, "row")),
            check_vma=False,
        )(snapshots, tail_sensors, shift_offsets, start_basis)

    return step
```

```python
import functools

import jax
import jax.numpy as jnp
from jax import lax
from jax.experimental import pallas as pl
from jax.experimental.pallas import tpu as pltpu
from jax.sharding import PartitionSpec as P

MESH = pl.DeviceIdType.MESH
HALF_ROOT = 0.7071067811865476
NT = (((1,), (1,)), ((), ()))
NN = (((1,), (0,)), ((), ()))
CHUNK = 128
GROUP = 8


def split(value):
    high = value.astype(jnp.bfloat16)
    return high, (value - high.astype(jnp.float32)).astype(jnp.bfloat16)


def dot(left, right, dims):
    return lax.dot_general(left, right, dims, preferred_element_type=jnp.float32)


def dot3(left, right, dims):
    left_high, left_low = split(left)
    right_high, right_low = split(right)
    return dot(left_high, right_high, dims) + (
        dot(left_low, right_high, dims) + dot(left_high, right_low, dims)
    )


def dot_full(left, right, dims):
    return lax.dot_general(
        left,
        right,
        dims,
        precision=lax.Precision.HIGHEST,
        preferred_element_type=jnp.float32,
    )


def inverse_factor(gram):
    k = gram.shape[0]
    row_ids = lax.broadcasted_iota(jnp.int32, (k, k), 0)
    col_ids = lax.broadcasted_iota(jnp.int32, (k, k), 1)
    eye = jnp.where(row_ids == col_ids, 1.0, 0.0).astype(jnp.float32)
    table = jnp.concatenate([gram, eye], axis=1)
    tall = lax.broadcasted_iota(jnp.int32, (k, 2 * k), 0)
    for j in range(0, k, GROUP):
        columns = [jnp.broadcast_to(table[:, j + a : j + a + 1], (k, 2 * k)) for a in range(GROUP)]
        rows = [table[j + a : j + a + 1, :] for a in range(GROUP)]
        for a in range(GROUP):
            inverse = 1.0 / columns[a][j + a : j + a + 1, :]
            scaled = rows[a] * inverse
            for c in range(a + 1, GROUP):
                shared = columns[a][j + c : j + c + 1, :]
                factor = columns[c][j + a : j + a + 1, :] * inverse
                columns[c] = columns[c] - columns[a] * factor
                rows[c] = rows[c] - scaled * shared
            table = table - jnp.where(tall > j + a, columns[a] * scaled, 0.0)
    pivots = jnp.sum(jnp.where(row_ids == col_ids, table[:, :k], 0.0), axis=1, keepdims=True)
    return table[:, k:] * lax.rsqrt(pivots)


def kernel(
    n_row, n_shift, m,
    snap_ref, tail_ref, offs_ref, start_ref,
    cov_ref, basis_ref,
    xb, xf, rf, prow, pcol, cov, offs_v, offs_s,
    t1, rs1, ag1, t2, rs2, ag2, g1, g2,
    x_send, x_recv, o_send, o_recv,
    rs1_send, rs1_recv, ag1_send, ag1_recv,
    rs2_send, rs2_recv, ag2_send, ag2_recv,
    g1_send, g1_recv, g2_send, g2_recv, local_sem, cov_sem,
):
    me = lax.axis_index("row")
    col = lax.axis_index("shift")
    rows = snap_ref.shape[0]
    tail = tail_ref.shape[0]
    k = start_ref.shape[0]
    cols = m // n_shift
    pair = me % 2
    mate = me + 1 - 2 * pair

    barrier = pltpu.get_barrier_semaphore()
    for d in range(1, n_row):
        pl.semaphore_signal(barrier, inc=1, device_id={"row": (me + d) % n_row}, device_id_type=MESH)
    for d in range(1, n_shift):
        pl.semaphore_signal(barrier, inc=1, device_id={"shift": (col + d) % n_shift}, device_id_type=MESH)
    pl.semaphore_wait(barrier, n_row + n_shift - 2)

    sends = []

    def remote(src, dst, send, recv, axis, index):
        return pltpu.make_async_remote_copy(
            src_ref=src, dst_ref=dst, send_sem=send, recv_sem=recv,
            device_id={axis: index}, device_id_type=MESH,
        )

    def push(*args):
        copy = remote(*args)
        copy.start()
        sends.append(copy)

    def block(index):
        return xb.at[pl.ds(pl.multiple_of(index * rows, rows), rows)]

    lanes_of = lax.broadcasted_iota(jnp.int32, (1, 128), 1)
    listed = jnp.zeros((1, 128), jnp.int32)
    for j in range(offs_ref.shape[0]):
        listed = jnp.where(lanes_of == j, offs_ref[j], listed)
    offs_v[col] = listed

    for d in range(1, n_shift):
        push(offs_v.at[col], offs_v.at[col], o_send.at[d], o_recv.at[col], "shift", (col + d) % n_shift)
    half_rows = rows // 2

    def part(index, h):
        return xb.at[pl.ds(pl.multiple_of(index * rows + h * half_rows, half_rows), half_rows)]

    def own_part(h):
        return snap_ref.at[pl.ds(h * half_rows, half_rows)]

    used = []

    def give(src, index, h, peer):
        push(src, part(index, h), x_send.at[len(used)], x_recv.at[2 * index + h], "row", peer)
        used.append(1)

    def take(index, h):
        remote(own_part(h), part(index, h), x_send.at[0], x_recv.at[2 * index + h], "row", mate).wait_recv()

    square = n_row == 8
    if square:
        quarter = me // 2
        along = 2 * (quarter + 1 - 2 * (quarter % 2)) + pair
        across = 2 * (quarter + 2 - 4 * (quarter // 2)) + pair
        opposite = 2 * (3 - quarter) + pair
        for h, peer in ((0, along), (1, across), (1, along), (0, across)):
            give(own_part(h), me, h, peer)
    else:
        for d in range(1, n_row // 2):
            for h in range(2):
                give(own_part(h), me, h, (me + 2 * d) % n_row)
    for h in range(2):
        give(own_part(h), me, h, mate)
    own_copy = pltpu.make_async_copy(snap_ref, block(me), local_sem.at[0])
    own_copy.start()
    tail_copy = pltpu.make_async_copy(tail_ref, xb.at[pl.ds(m, tail)], local_sem.at[1])
    tail_copy.start()

    flip_rows = lax.broadcasted_iota(jnp.int32, (CHUNK, CHUNK), 0)
    flip_cols = lax.broadcasted_iota(jnp.int32, (CHUNK, CHUNK), 1)
    flip = jnp.where(flip_rows + flip_cols == CHUNK - 1, 1.0, 0.0).astype(jnp.bfloat16)

    def spread(first, count):
        def one(c, carry):
            at = pl.multiple_of(first + c * CHUNK, CHUNK)
            value = xb[pl.ds(at, CHUNK), :]
            plain = value.astype(jnp.float32)
            back = dot(flip, value, NN)
            other = pl.multiple_of(m + tail - CHUNK - at, CHUNK)
            half = plain.shape[1] // 2
            xf[0, pl.ds(at, CHUNK), :] = plain[:, :half]
            xf[1, pl.ds(at, CHUNK), :] = plain[:, half:]
            rf[0, pl.ds(other, CHUNK), :] = back[:, :half]
            rf[1, pl.ds(other, CHUNK), :] = back[:, half:]
            return carry

        lax.fori_loop(0, count // CHUNK, one, 0)

    tail_copy.wait()
    spread(m, tail)
    own_copy.wait()
    spread(me * rows, rows)

    def swap(index):
        return index + 1 - 2 * (index % 2)

    if square:
        for index, h, onward in (
            (along, 0, across), (across, 1, along), (along, 1, None),
            (across, 0, None), (opposite, 0, None), (opposite, 1, None),
        ):
            take(index, h)
            if onward is not None:
                give(part(index, h), index, h, onward)
            give(part(index, h), index, h, mate)
            if index is not opposite and onward is None:
                spread(index * rows, rows)
        spread(opposite * rows, rows)
        others = [along, across, opposite]
    else:
        others = [(me + n_row - 2 * d) % n_row for d in range(1, n_row // 2)]
        for index in others:
            for h in range(2):
                take(index, h)
                give(part(index, h), index, h, mate)
            spread(index * rows, rows)
    for index in [me] + others:
        for h in range(2):
            take(swap(index), h)
        spread(swap(index) * rows, rows)

    for d in range(1, n_shift):
        src = (col + n_shift - d) % n_shift
        remote(offs_v.at[src], offs_v.at[src], o_send.at[d], o_recv.at[src], "shift", src).wait_recv()
    to_scalar = pltpu.make_async_copy(offs_v, offs_s, local_sem.at[2])
    to_scalar.start()
    to_scalar.wait()

    snaps = xf.shape[2]
    width = 2 * snaps
    per = prow.shape[1] // (width * n_shift)

    def fill(target, start, count):
        lower = start >= m // 2
        first = jnp.where(lower, 1, 0)
        second = 1 - first
        sign = jnp.where(lower, -1.0, 1.0).astype(jnp.float32)

        def one_shift(s, carry):
            offset = offs_s[s // per, 0, s % per]
            lanes = pl.multiple_of(s * width, width)
            for c in range(count // CHUNK):
                near = pl.ds(offset + start + c * CHUNK, CHUNK)
                far = pl.ds(tail - offset + start + c * CHUNK, CHUNK)
                left = (xf[first, near, :] + sign * rf[first, far, :]) * HALF_ROOT
                right = (xf[second, near, :] + sign * rf[second, far, :]) * (sign * HALF_ROOT)
                target[pl.ds(c * CHUNK, CHUNK), pl.ds(lanes, snaps)] = left.astype(jnp.bfloat16)
                target[pl.ds(c * CHUNK, CHUNK), pl.ds(pl.multiple_of(lanes + snaps, snaps), snaps)] = right.astype(jnp.bfloat16)
            return carry

        lax.fori_loop(0, per * n_shift, one_shift, 0)

    fill(prow, me * rows, rows)
    fill(pcol, col * cols, cols)

    normalizer = 1.0 / (snaps * per * n_shift)
    def scatter(value, out, landing, send, recv, axis, index, n):
        piece = k // n
        for p in range(n):
            out[p] = value[p * piece : (p + 1) * piece, :]
        for d in range(1, n):
            p = (index + d) % n
            push(out.at[p], landing.at[index], send.at[d], recv.at[index], axis, p)

    def collect(out, landing, held, send, recv, send2, recv2, axis, index, n):
        for d in range(1, n):
            p = (index + n - d) % n
            remote(out.at[p], landing.at[p], send.at[d], recv.at[p], axis, p).wait_recv()
        landing[index] = out[index]
        total = landing[0]
        for p in range(1, n):
            total = total + landing[p]
        held[index] = total
        for d in range(1, n):
            p = (index + d) % n
            push(held.at[index], held.at[index], send2.at[d], recv2.at[index], axis, p)

    def arrive(held, send, recv, axis, index, n):
        for d in range(1, n):
            p = (index + n - d) % n
            remote(held.at[p], held.at[p], send.at[d], recv.at[p], axis, p).wait_recv()

    def whole(held, n):
        return jnp.concatenate([held[p] for p in range(n)], axis=0)

    tiles = t1.shape[0]
    tile = cols // tiles

    def settle(c):
        collect(
            t1.at[c], rs1.at[c], ag1.at[c], rs1_send.at[c], rs1_recv.at[c],
            ag1_send.at[c], ag1_recv.at[c], "row", me, n_row,
        )

    start = start_ref[...]
    for c in range(tiles):
        at = pl.ds(c * tile, tile)
        cov[:, at] = dot(prow[...], pcol[at, :], NT) * normalizer
        scatter(
            dot3(start, cov[:, at], NN), t1.at[c], rs1.at[c],
            rs1_send.at[c], rs1_recv.at[c], "row", me, n_row,
        )
        if c >= 2:
            settle(c - 2)
    cov_copy = pltpu.make_async_copy(cov, cov_ref, cov_sem)
    cov_copy.start()
    for c in range(max(tiles - 2, 0), tiles):
        settle(c)
    for c in range(tiles):
        arrive(ag1.at[c], ag1_send.at[c], ag1_recv.at[c], "row", me, n_row)
    mapped = jnp.concatenate([whole(ag1.at[c], n_row) for c in range(tiles)], axis=1)

    g1[col] = dot_full(mapped, mapped, NT)
    for d in range(1, n_shift):
        push(g1.at[col], g1.at[col], g1_send.at[d], g1_recv.at[col], "shift", (col + d) % n_shift)
    scatter(dot3(mapped, cov[...], NT), t2, rs2, rs2_send, rs2_recv, "shift", col, n_shift)
    arrive(g1, g1_send, g1_recv, "shift", col, n_shift)
    collect(t2, rs2, ag2, rs2_send, rs2_recv, ag2_send, ag2_recv, "shift", col, n_shift)
    gram = g1[0]
    for p in range(1, n_shift):
        gram = gram + g1[p]
    first_inverse = inverse_factor(gram)
    arrive(ag2, ag2_send, ag2_recv, "shift", col, n_shift)
    mapped = dot_full(first_inverse, whole(ag2, n_shift), NN)

    g2[me] = dot_full(mapped, mapped, NT)
    for d in range(1, n_row):
        push(g2.at[me], g2.at[me], g2_send.at[d], g2_recv.at[me], "row", (me + d) % n_row)
    arrive(g2, g2_send, g2_recv, "row", me, n_row)
    gram = g2[0]
    for p in range(1, n_row):
        gram = gram + g2[p]
    basis_ref[...] = dot_full(inverse_factor(gram), mapped, NN)

    for copy in sends:
        copy.wait_send()
    cov_copy.wait()


def per_device(n_row, n_shift, m, snapshots, tail_sensors, shift_offsets, start_basis):
    rows = snapshots.shape[0]
    tail = tail_sensors.shape[0]
    k = start_basis.shape[0]
    cols = m // n_shift
    per = shift_offsets.shape[0]
    width = snapshots.shape[1] * snapshots.shape[2]
    tiles = max(cols // 256, 1)
    vmem = pl.BlockSpec(memory_space=pltpu.VMEM)
    f32, bf16 = jnp.float32, jnp.bfloat16
    dma = pltpu.SemaphoreType.DMA
    return pl.pallas_call(
        functools.partial(kernel, n_row, n_shift, m),
        out_shape=(
            jax.ShapeDtypeStruct((rows, cols), f32),
            jax.ShapeDtypeStruct((k, rows), f32),
        ),
        in_specs=[vmem, vmem, pl.BlockSpec(memory_space=pltpu.SMEM), vmem],
        out_specs=(pl.BlockSpec(memory_space=pl.ANY), vmem),
        scratch_shapes=[
            pltpu.VMEM((m + tail, width), bf16),
            pltpu.VMEM((2, m + tail, width // 2), f32),
            pltpu.VMEM((2, m + tail, width // 2), f32),
            pltpu.VMEM((rows, width * per * n_shift), bf16),
            pltpu.VMEM((cols, width * per * n_shift), bf16),
            pltpu.VMEM((rows, cols), f32),
            pltpu.VMEM((n_shift, 1, 128), jnp.int32),
            pltpu.SMEM((n_shift, 1, 128), jnp.int32),
            pltpu.VMEM((tiles, n_row, k // n_row, cols // tiles), f32),
            pltpu.VMEM((tiles, n_row, k // n_row, cols // tiles), f32),
            pltpu.VMEM((tiles, n_row, k // n_row, cols // tiles), f32),
            pltpu.VMEM((n_shift, k // n_shift, rows), f32),
            pltpu.VMEM((n_shift, k // n_shift, rows), f32),
            pltpu.VMEM((n_shift, k // n_shift, rows), f32),
            pltpu.VMEM((n_shift, k, k), f32),
            pltpu.VMEM((n_row, k, k), f32),
            dma((2 * n_row,)), dma((2 * n_row,)),
            dma((n_shift,)), dma((n_shift,)),
            dma((tiles, n_row)), dma((tiles, n_row)), dma((tiles, n_row)), dma((tiles, n_row)),
            dma((n_shift,)), dma((n_shift,)), dma((n_shift,)), dma((n_shift,)),
            dma((n_shift,)), dma((n_shift,)), dma((n_row,)), dma((n_row,)),
            dma((3,)), dma,
        ],
        compiler_params=pltpu.CompilerParams(
            collective_id=0, has_side_effects=True, vmem_limit_bytes=32 * 1024 * 1024
        ),
    )(snapshots.reshape(rows, width), tail_sensors.reshape(tail, width), shift_offsets, start_basis)


def solution(mesh):
    n_row, n_shift = mesh.shape["row"], mesh.shape["shift"]

    def step(snapshots, tail_sensors, shift_offsets, start_basis):
        m = snapshots.shape[0]
        return jax.shard_map(
            functools.partial(per_device, n_row, n_shift, m),
            mesh=mesh,
            in_specs=(P("row", None, None), P(), P("shift"), P(None, "row")),
            out_specs=(P("row", "shift"), P(None, "row")),
            check_vma=False,
        )(snapshots, tail_sensors, shift_offsets, start_basis)

    return step
```
